32 devices in a mesh: ctx: 16 (over z, y, core), head: 2 (over x).
Axes of the slice: x: 2, y: 2, z: 4, core: 2. Of those that a mesh axis runs over, the one named last changes fastest.
Arguments:
- queries: bfloat16 [2048, 2048], P('ctx', 'head'), may hold values from -100 to 100
- keys: bfloat16 [2048, 2048], P('ctx', 'head'), may hold values from -50 to 50
- values: bfloat16 [2048, 2048], P('ctx', 'head'), may hold values from -6 to 6
- out_weight: bfloat16 [2048, 4096], P('head'), may hold values from -0.125 to 0.125
- mixed_grad: bfloat16 [2048, 4096], P('ctx', 'head'), may hold values from -6 to 6
- lengths: int32 [16], replicated, may hold values from 1 to 384, 2048 in all
- dilation: int32 [16], P('head'), may hold values from 1 to 8
Outputs:
- mixed: bfloat16 [2048, 4096], P('ctx', 'head')
- grad_queries: bfloat16 [2048, 2048], P('ctx', 'head')
- grad_keys: bfloat16 [2048, 2048], P('ctx', 'head')
- grad_values: bfloat16 [2048, 2048], P('ctx', 'head')
The draws below stay inside these ranges and needn't reach their ends.
Inputs may be any that keep to these rules, and one draw needn't show every extreme that they name: The lengths sum to 2048, and the longest document has exactly 384 tokens.
All inputs are finite; a program needn't handle non-finite values.
Results may differ from the reference program's by a relative error of at most 0.029.
Values may be sent and summed in bfloat16 or wider, within the bound.
A program may use at most 64 MiB of HBM per device.

```python
import math
import jax
import jax.numpy as jnp
import numpy as np
from jax import lax

D = 4096
HEADS = 16
HD = 128
HALF = 32
MAXD = 8
TOK_DEV = 128
TOKENS = 2048
DOCS = 16


def draw_queries(key, part):
    drawn = jax.random.normal(jax.random.fold_in(key, 11), (TOKENS, HEADS * HD), jnp.float32)
    return drawn.astype(jnp.bfloat16)


def draw_keys(key, part):
    drawn = jax.random.normal(jax.random.fold_in(key, 23), (TOKENS, HEADS * HD), jnp.float32)
    return drawn.astype(jnp.bfloat16)


def plant(entries, stream_key, smallest, high):
    shape = entries.shape
    spot = [jax.random.randint(jax.random.fold_in(stream_key, axis), (), 0, shape[axis]) for axis in range(len(shape))]
    entries = entries.at[tuple(spot)].set(smallest)
    longest = shape.index(max(shape))
    spot[longest] = (spot[longest] + 1) % shape[longest]
    return entries.at[tuple(spot)].set(high)


def block_scale(own_key, dims, shards, smallest, high):
    def one(axis_at, blocks):
        draws = jax.random.uniform(jax.random.fold_in(jax.random.fold_in(own_key, 6), axis_at), (blocks,), jnp.float32, smallest / len(shards), high / len(shards))
        return jnp.repeat(jnp.exp(draws), dims[axis_at] // blocks).reshape((-1,) + (1,) * (len(dims) - axis_at - 1))

    factor_of = one(*shards[0])
    for cut in shards[1:]:
        factor_of = factor_of * one(*cut)
    return factor_of


def split_up(amount, total, most, slope):
    portions = [(1 << 20) // math.isqrt(rank ** slope) + 1 for rank in range(2, amount + 1)]
    spare, given = total - most - (amount - 1), [1] * (amount - 1)
    while spare > 0:
        free = [i for i in range(amount - 1) if given[i] < most]
        pool, budget = sum([portions[i] for i in free]), spare
        for i in free:
            extra = min(most - given[i], max(1, budget * portions[i] // pool), spare)
            given[i] = given[i] + extra
            spare = spare - extra
    return np.array([most] + given)


def ragged(stream_key, amount, total, most, skew):
    if amount == 2:
        one = jax.random.randint(stream_key, (), max(1, total - most), min(most, total - 1) + 1)
        return jnp.stack([one, total - one])
    sizes = jnp.asarray(split_up(amount, total, most, skew), jnp.int32)
    twos = (amount - 1) // 2
    source_of, taker = sizes[1:1 + 2 * twos:2], sizes[2:2 + 2 * twos:2]
    room = jnp.minimum(source_of - 1, most - taker)
    moved = jax.random.randint(jax.random.fold_in(stream_key, 1), (twos,), 0, 1 << 20) % (room + 1)
    sizes = sizes.at[1:1 + 2 * twos:2].set(source_of - moved).at[2:2 + 2 * twos:2].set(taker + moved)
    return sizes[jax.random.permutation(jax.random.fold_in(stream_key, 2), amount)]


def noise(key, shape, spread, bound, shards=(), kind=jnp.bfloat16):
    values = jax.random.normal(key, shape, jnp.float32) * spread
    if len(shards) > 0:
        values = block_scale(key, shape, shards, -0.22, 0.18) * values
    return jnp.clip(values, min=-bound, max=bound).astype(kind)


def setup_inputs(seed: int = 0) -> dict:
    key_of = jax.random.split(jax.random.key(seed), 8)
    return {
        "queries": draw_queries(jax.random.fold_in(key_of[7], 71), 0),
        "keys": draw_keys(jax.random.fold_in(key_of[7], 71), 0),
        "values": noise(key_of[2], (TOKENS, HEADS * HD), 1.0, 6.0, ((0, 16), (1, 2))),
        "out_weight": noise(key_of[3], (HEADS * HD, D), (HEADS * HD) ** -0.5, 0.125, ((0, 2),)),
        "mixed_grad": noise(key_of[4], (TOKENS, D), 1.0, 6.0, ((0, 16), (1, 2))),
        "lengths": ragged(key_of[5], DOCS, TOKENS, HALF * MAXD + TOK_DEV, 2).astype(jnp.int32),
        "dilation": plant(jax.random.randint(key_of[6], (HEADS,), 1, MAXD + 1), jax.random.fold_in(key_of[6], 1), 1, MAXD).astype(jnp.int32),
    }


def segment_of(positions, lengths):
    boundary = jnp.cumsum(lengths).astype(jnp.int32)
    return jnp.sum((positions[:, None] >= boundary[None, :]).astype(jnp.int32), axis=1)


def allowed(query_pos, key_pos, query_seg, key_seg, dilation, reach, total):
    offset_grid = query_pos[:, None] - key_pos[None, :]
    common = (query_seg[:, None] == key_seg[None, :]) & (key_pos[None, :] >= 0) & (key_pos[None, :] < total)
    common = common & (query_pos[:, None] >= 0) & (query_pos[:, None] < total)
    stride = dilation[:, None, None]
    within = (jnp.abs(offset_grid)[None] <= reach * stride) & (jnp.remainder(offset_grid[None], stride) == 0)
    return within & common[None]


def reference(queries, keys, values, out_weight, mixed_grad, lengths, dilation):
    total = queries.shape[0]
    margin = HALF * MAXD
    factor = HD ** -0.5
    window = TOK_DEV + 2 * margin
    blocks = total // TOK_DEV
    grad_attention = jnp.dot(mixed_grad, out_weight.T, preferred_element_type=jnp.float32).astype(jnp.bfloat16)

    def by_head(array):
        return array.reshape(total, HEADS, HD).transpose(1, 0, 2)

    def one_head(item):
        query_rows, key_rows, value_rows, grad_rows, spacing = item
        padding = ((margin, margin), (0, 0))
        key_padded = jnp.pad(key_rows, padding)
        value_padded = jnp.pad(value_rows, padding)
        zeros_pad = jnp.zeros((total + 2 * margin, HD), jnp.float32)

        def step(carry, block):
            key_acc, value_acc = carry
            start = (block * TOK_DEV).astype(jnp.int32)
            query_block = lax.dynamic_slice_in_dim(query_rows, start, TOK_DEV, 0)
            grad_block = lax.dynamic_slice_in_dim(grad_rows, start, TOK_DEV, 0)
            key_window = lax.dynamic_slice_in_dim(key_padded, start, window, 0)
            value_window = lax.dynamic_slice_in_dim(value_padded, start, window, 0)
            query_pos = start + jnp.arange(TOK_DEV, dtype=jnp.int32)
            key_pos = start - margin + jnp.arange(window, dtype=jnp.int32)
            mask = allowed(query_pos, key_pos, segment_of(query_pos, lengths), segment_of(key_pos, lengths), spacing[None], HALF, total)[0]
            scores = jnp.dot(query_block, key_window.T, preferred_element_type=jnp.float32) * factor
            top = jnp.max(jnp.where(mask, scores, -jnp.inf), axis=1)
            log_total = top + jnp.log(jnp.sum(jnp.where(mask, jnp.exp(scores - top[:, None]), 0.0), axis=1))
            weights = jnp.where(mask, jnp.exp(scores - log_total[:, None]), 0.0)
            probs = weights.astype(jnp.bfloat16)
            attention = jnp.dot(probs, value_window, preferred_element_type=jnp.float32).astype(jnp.bfloat16)
            delta = jnp.sum(grad_block.astype(jnp.float32) * attention.astype(jnp.float32), axis=1)
            grad_prob = jnp.dot(grad_block, value_window.T, preferred_element_type=jnp.float32)
            slopes = (weights * (grad_prob - delta[:, None])).astype(jnp.bfloat16)
            grad_query = (jnp.dot(slopes, key_window, preferred_element_type=jnp.float32) * factor).astype(jnp.bfloat16)
            key_term = jnp.dot(slopes.T, query_block, preferred_element_type=jnp.float32) * factor
            value_term = jnp.dot(probs.T, grad_block, preferred_element_type=jnp.float32)
            key_acc = lax.dynamic_update_slice_in_dim(key_acc, lax.dynamic_slice_in_dim(key_acc, start, window, 0) + key_term, start, 0)
            value_acc = lax.dynamic_update_slice_in_dim(value_acc, lax.dynamic_slice_in_dim(value_acc, start, window, 0) + value_term, start, 0)
            return (key_acc, value_acc), (attention, grad_query)

        (key_acc, value_acc), (attention, grad_query) = lax.scan(step, (zeros_pad, zeros_pad), jnp.arange(blocks, dtype=jnp.int32))
        grad_key = key_acc[margin:margin + total].astype(jnp.bfloat16)
        grad_value = value_acc[margin:margin + total].astype(jnp.bfloat16)
        return attention.reshape(total, HD), grad_query.reshape(total, HD), grad_key, grad_value

    results = lax.map(one_head, (by_head(queries), by_head(keys), by_head(values), by_head(grad_attention), dilation))

    def flat(array):
        return array.transpose(1, 0, 2).reshape(total, HEADS * HD)

    attention = flat(results[0])
    mixed = jnp.dot(attention, out_weight, preferred_element_type=jnp.float32).astype(jnp.bfloat16)
    return mixed, flat(results[1]), flat(results[2]), flat(results[3])
```

```python
import functools
import jax
import jax.numpy as jnp
from jax import lax
from jax.experimental import pallas as pl
from jax.experimental.pallas import tpu as pltpu
from jax.sharding import PartitionSpec as P

HALF = 32
MAXD = 8
FAR = 1e6
NEG = -1e30


def attend_kernel(
    row_count, total, factor, first, index_ref, bound_ref, inv_ref,
    q_ref, go_ref, own_ref, a_ref, b_ref, po_ref, pa_ref,
    att_ref, gq_ref, own_t, a_t, b_t, po_t, pa_t, dist,
):
    slabs = (own_ref, a_ref, b_ref, po_ref, pa_ref)
    outs = (own_t, a_t, b_t, po_t, pa_t)

    @pl.when(pl.program_id(0) == 0)
    def _():
        me = index_ref[0]
        sign = 1 - 2 * lax.rem(me, 2)
        ndocs = bound_ref.shape[0]

        def segment(pos):
            seg = jnp.zeros(pos.shape, jnp.int32)
            for n in range(ndocs):
                seg = seg + (pos >= bound_ref[n]).astype(jnp.int32)
            return seg

        qpos = me * row_count + lax.broadcasted_iota(jnp.int32, (1, row_count), 1)
        qseg = segment(qpos)
        for i, off in enumerate((0, 2, -2, 1, -1)):
            kpos = (me + sign * off) * row_count + lax.broadcasted_iota(
                jnp.int32, (row_count, row_count), 0
            )
            same = (segment(kpos) == qseg) & (kpos >= 0) & (kpos < total)
            gap = jnp.abs(kpos - qpos).astype(jnp.float32)
            dist[pl.ds(i * row_count, row_count), :] = jnp.where(same, gap, FAR)

    inv = inv_ref[first + pl.program_id(0)]
    steps = dist[...] * inv
    whole = jnp.floor(steps + 0.5)
    mask = (whole <= HALF) & (jnp.abs(steps - whole) < 0.01)
    q = q_ref[...]
    go = go_ref[...]
    k = jnp.concatenate([r[0] for r in slabs], axis=0)
    v = jnp.concatenate([r[1] for r in slabs], axis=0)
    nt = (((1,), (1,)), ((), ()))
    tn = (((0,), (0,)), ((), ()))
    f32 = jnp.float32
    scores = lax.dot_general(k, q, nt, preferred_element_type=f32) * factor
    scores = jnp.where(mask, scores, NEG)
    top = jnp.max(scores, axis=0, keepdims=True)
    e = jnp.exp(scores - top)
    w = e * (1.0 / jnp.sum(e, axis=0, keepdims=True))
    p = w.astype(jnp.bfloat16)
    gp = lax.dot_general(v, go, nt, preferred_element_type=f32)
    delta = jnp.sum(w * gp, axis=0, keepdims=True)
    s = (w * (gp - delta)).astype(jnp.bfloat16)
    att_ref[...] = lax.dot_general(p, v, tn, preferred_element_type=f32).astype(jnp.bfloat16)
    gq_ref[...] = (
        lax.dot_general(s, k, tn, preferred_element_type=f32) * factor
    ).astype(jnp.bfloat16)
    kt = (jnp.dot(s, q, preferred_element_type=f32) * factor).astype(jnp.bfloat16)
    vt = jnp.dot(p, go, preferred_element_type=f32).astype(jnp.bfloat16)
    for i, out in enumerate(outs):
        out[0] = kt[i * row_count : (i + 1) * row_count]
        out[1] = vt[i * row_count : (i + 1) * row_count]


def attend(index, bounds, inv, q, go, slabs, first, total, factor, width):
    rows, cols = q.shape[0], slabs[0].shape[2]
    heads = cols // width
    smem = pl.BlockSpec(memory_space=pltpu.SMEM)
    shared = pl.BlockSpec((rows, width), lambda h: (0, first + h))
    flat = pl.BlockSpec((rows, width), lambda h: (0, h))
    pair = pl.BlockSpec((2, rows, width), lambda h: (0, 0, h))
    one = jax.ShapeDtypeStruct((rows, cols), jnp.bfloat16)
    two = jax.ShapeDtypeStruct((2, rows, cols), jnp.bfloat16)
    return pl.pallas_call(
        functools.partial(attend_kernel, rows, total, factor, first),
        grid=(heads,),
        in_specs=[smem, smem, smem, shared, shared] + [pair] * 5,
        out_specs=[flat, flat] + [pair] * 5,
        out_shape=[one, one] + [two] * 5,
        scratch_shapes=[pltpu.VMEM((5 * rows, rows), jnp.float32)],
        compiler_params=pltpu.CompilerParams(dimension_semantics=("arbitrary",)),
        cost_estimate=pl.CostEstimate(
            flops=heads * 6 * 2 * 5 * rows * rows * width * 8,
            bytes_accessed=24 * 2 * rows * cols,
            transcendentals=heads * 5 * rows * rows,
        ),
    )(index, bounds, inv, q, go, *slabs)


def per_device(queries, keys, values, out_weight, mixed_grad, lengths, dilation):
    rows = queries.shape[0]
    local_heads = dilation.shape[0]
    width = queries.shape[1] // local_heads
    factor = width ** (-0.5)
    count = lax.axis_size("ctx")
    sides = lax.axis_size("head")
    total = rows * count
    assert 2 * rows >= HALF * MAXD and count % 2 == 0
    index = lax.axis_index("ctx").astype(jnp.int32).reshape(1)
    bounds = jnp.cumsum(lengths).astype(jnp.int32)
    inv = 1.0 / dilation.astype(jnp.float32)

    inward = [
        (j, t) for j in range(count) for t in [j - 2 if j % 2 == 0 else j + 2] if 0 <= t < count
    ]
    outward = [(t, j) for j, t in inward]
    swapped = [(j, j ^ 1) for j in range(count)]

    def move(x, pairs):
        return lax.ppermute(x, "ctx", pairs)

    groups = 2 if local_heads % 2 == 0 else 1
    gh = local_heads // groups
    cut = [slice(g * gh * width, (g + 1) * gh * width) for g in range(groups)]
    half = mixed_grad.shape[1]
    if sides == 2:
        other = lax.ppermute(mixed_grad, "head", [(0, 1), (1, 0)])
        left = lax.axis_index("head") == 0
        grad_full = jnp.concatenate(
            [jnp.where(left, mixed_grad, other), jnp.where(left, other, mixed_grad)], axis=1
        )
    else:
        grad_full = lax.all_gather(mixed_grad, "head", axis=1, tiled=True)
    stacks = []
    for g in range(groups):
        own = jnp.stack([keys[:, cut[g]], values[:, cut[g]]])
        a = move(own, inward)
        stacks.append((own, a, move(own, outward), move(own, swapped), move(a, swapped)))
    grad_attention = lax.dot_general(
        grad_full, out_weight, (((1,), (1,)), ((), ())), preferred_element_type=jnp.float32
    ).astype(jnp.bfloat16)

    atts, gqs, gkvs = [], [], []
    f32 = jnp.float32
    for g in range(groups):
        att, gq, own_t, a_t, b_t, po_t, pa_t = attend(
            index, bounds, inv, queries, grad_attention, stacks[g], g * gh, total, factor, width
        )
        pa_back = move(pa_t, swapped)
        b_back = move(b_t, inward)
        po_back = move(po_t, swapped)
        a_sum = (a_t.astype(f32) + pa_back.astype(f32)).astype(jnp.bfloat16)
        a_back = move(a_sum, outward)
        gkvs.append(
            (
                own_t.astype(f32) + po_back.astype(f32) + b_back.astype(f32) + a_back.astype(f32)
            ).astype(jnp.bfloat16)
        )
        atts.append(att)
        gqs.append(gq)
    attention = jnp.concatenate(atts, axis=1)
    partial = jnp.dot(attention, out_weight, preferred_element_type=f32)
    if sides == 2:
        lo, hi = partial[:, :half], partial[:, half:]
        away = jnp.where(left, hi, lo).astype(jnp.bfloat16)
        came = lax.ppermute(away, "head", [(0, 1), (1, 0)])
        mixed = (jnp.where(left, lo, hi) + came.astype(f32)).astype(jnp.bfloat16)
    else:
        mixed = lax.psum_scatter(
            partial.astype(jnp.bfloat16), "head", scatter_dimension=1, tiled=True
        )
    gkv = jnp.concatenate(gkvs, axis=2)
    return mixed, jnp.concatenate(gqs, axis=1), gkv[0], gkv[1]


def solution(mesh):
    both = P("ctx", "head")
    return jax.shard_map(
        per_device,
        mesh=mesh,
        in_specs=(both, both, both, P("head", None), both, P(), P("head")),
        out_specs=(both, both, both, both),
        check_vma=False,
    )
```

```python
import functools
import jax
import jax.numpy as jnp
from jax import lax
from jax.experimental import pallas as pl
from jax.experimental.pallas import tpu as pltpu
from jax.sharding import PartitionSpec as P

HALF = 32
MAXD = 8
FAR = 1e6
NEG = -1e30


def attend_kernel(
    row_count, total, factor, first, index_ref, length_ref, dilation_ref,
    q_ref, go_ref, own_ref, a_ref, b_ref, po_ref, pa_ref,
    att_ref, gq_ref, own_t, a_t, b_t, po_t, pa_t, dist,
):
    slabs = (own_ref, a_ref, b_ref, po_ref, pa_ref)
    outs = (own_t, a_t, b_t, po_t, pa_t)

    @pl.when(pl.program_id(0) == 0)
    def _():
        me = index_ref[0]
        sign = 1 - 2 * lax.rem(me, 2)
        ends = [length_ref[0]]
        for n in range(1, length_ref.shape[0]):
            ends.append(ends[-1] + length_ref[n])

        def segment(pos):
            seg = jnp.zeros(pos.shape, jnp.int32)
            for end in ends:
                seg = seg + (pos >= end).astype(jnp.int32)
            return seg

        qpos = me * row_count + lax.broadcasted_iota(jnp.int32, (1, row_count), 1)
        qseg = segment(qpos)
        for i, off in enumerate((0, 2, -2, 1, -1)):
            kpos = (me + sign * off) * row_count + lax.broadcasted_iota(
                jnp.int32, (row_count, row_count), 0
            )
            same = (segment(kpos) == qseg) & (kpos >= 0) & (kpos < total)
            gap = jnp.abs(kpos - qpos).astype(jnp.float32)
            dist[pl.ds(i * row_count, row_count), :] = jnp.where(same, gap, FAR)

    spacing = jnp.full((1, row_count), dilation_ref[first + pl.program_id(0)], jnp.int32)
    inv = 1.0 / spacing.astype(jnp.float32)
    steps = dist[...] * inv
    whole = jnp.floor(steps + 0.5)
    mask = (whole <= HALF) & (jnp.abs(steps - whole) < 0.01)
    q = q_ref[...]
    go = go_ref[...]
    k = jnp.concatenate([r[0] for r in slabs], axis=0)
    v = jnp.concatenate([r[1] for r in slabs], axis=0)
    nt = (((1,), (1,)), ((), ()))
    tn = (((0,), (0,)), ((), ()))
    f32 = jnp.float32
    scores = lax.dot_general(k, q, nt, preferred_element_type=f32) * factor
    scores = jnp.where(mask, scores, NEG)
    top = jnp.max(scores, axis=0, keepdims=True)
    e = jnp.exp(scores - top)
    w = e * (1.0 / jnp.sum(e, axis=0, keepdims=True))
    p = w.astype(jnp.bfloat16)
    gp = lax.dot_general(v, go, nt, preferred_element_type=f32)
    delta = jnp.sum(w * gp, axis=0, keepdims=True)
    s = (w * (gp - delta)).astype(jnp.bfloat16)
    att_ref[...] = lax.dot_general(p, v, tn, preferred_element_type=f32).astype(jnp.bfloat16)
    gq_ref[...] = (
        lax.dot_general(s, k, tn, preferred_element_type=f32) * factor
    ).astype(jnp.bfloat16)
    kt = (jnp.dot(s, q, preferred_element_type=f32) * factor).astype(jnp.bfloat16)
    vt = jnp.dot(p, go, preferred_element_type=f32).astype(jnp.bfloat16)
    for i, out in enumerate(outs):
        out[0] = kt[i * row_count : (i + 1) * row_count]
        out[1] = vt[i * row_count : (i + 1) * row_count]


def attend(index, lengths, dilation, q, go, slabs, first, total, factor, width):
    rows, cols = q.shape[0], slabs[0].shape[2]
    heads = cols // width
    smem = pl.BlockSpec(memory_space=pltpu.SMEM)
    shared = pl.BlockSpec((rows, width), lambda h: (0, first + h))
    flat = pl.BlockSpec((rows, width), lambda h: (0, h))
    pair = pl.BlockSpec((2, rows, width), lambda h: (0, 0, h))
    one = jax.ShapeDtypeStruct((rows, cols), jnp.bfloat16)
    two = jax.ShapeDtypeStruct((2, rows, cols), jnp.bfloat16)
    return pl.pallas_call(
        functools.partial(attend_kernel, rows, total, factor, first),
        grid=(heads,),
        in_specs=[smem, smem, smem, shared, shared] + [pair] * 5,
        out_specs=[flat, flat] + [pair] * 5,
        out_shape=[one, one] + [two] * 5,
        scratch_shapes=[pltpu.VMEM((5 * rows, rows), jnp.float32)],
        compiler_params=pltpu.CompilerParams(dimension_semantics=("arbitrary",)),
        cost_estimate=pl.CostEstimate(
            flops=heads * 6 * 2 * 5 * rows * rows * width * 8,
            bytes_accessed=24 * 2 * rows * cols,
            transcendentals=heads * 5 * rows * rows,
        ),
    )(index, lengths, dilation, q, go, *slabs)


def per_device(queries, keys, values, out_weight, mixed_grad, lengths, dilation):
    rows = queries.shape[0]
    local_heads = dilation.shape[0]
    width = queries.shape[1] // local_heads
    factor = width ** (-0.5)
    count = lax.axis_size("ctx")
    sides = lax.axis_size("head")
    total = rows * count
    assert 2 * rows >= HALF * MAXD and count % 2 == 0
    index = lax.axis_index("ctx").astype(jnp.int32).reshape(1)

    inward = [
        (j, t) for j in range(count) for t in [j - 2 if j % 2 == 0 else j + 2] if 0 <= t < count
    ]
    outward = [(t, j) for j, t in inward]
    swapped = [(j, j ^ 1) for j in range(count)]

    def move(x, pairs):
        return lax.ppermute(x, "ctx", pairs)

    groups = 1
    gh = local_heads // groups
    cut = [slice(g * gh * width, (g + 1) * gh * width) for g in range(groups)]
    half = mixed_grad.shape[1]
    if sides == 2:
        other = lax.ppermute(mixed_grad, "head", [(0, 1), (1, 0)])
        left = lax.axis_index("head") == 0
        grad_full = jnp.concatenate(
            [jnp.where(left, mixed_grad, other), jnp.where(left, other, mixed_grad)], axis=1
        )
    else:
        grad_full = lax.all_gather(mixed_grad, "head", axis=1, tiled=True)
    stacks = []
    for g in range(groups):
        own = jnp.stack([keys[:, cut[g]], values[:, cut[g]]])
        a = move(own, inward)
        stacks.append((own, a, move(own, outward), move(own, swapped), move(a, swapped)))
    grad_attention = lax.dot_general(
        grad_full, out_weight, (((1,), (1,)), ((), ())), preferred_element_type=jnp.float32
    ).astype(jnp.bfloat16)

    atts, gqs, gkvs = [], [], []
    f32 = jnp.float32
    for g in range(groups):
        att, gq, own_t, a_t, b_t, po_t, pa_t = attend(
            index, lengths, dilation, queries, grad_attention, stacks[g], g * gh, total, factor, width
        )
        pa_back = move(pa_t, swapped)
        b_back = move(b_t, inward)
        po_back = move(po_t, swapped)
        a_sum = (a_t.astype(f32) + pa_back.astype(f32)).astype(jnp.bfloat16)
        a_back = move(a_sum, outward)
        terms = (own_t, po_back, b_back, a_back)
        gkvs.append(
            [sum(term[i].astype(f32) for term in terms).astype(jnp.bfloat16) for i in range(2)]
        )
        atts.append(att)
        gqs.append(gq)
    attention = jnp.concatenate(atts, axis=1)
    partial = jnp.dot(attention, out_weight, preferred_element_type=f32)
    if sides == 2:
        lo, hi = partial[:, :half], partial[:, half:]
        away = jnp.where(left, hi, lo).astype(jnp.bfloat16)
        came = lax.ppermute(away, "head", [(0, 1), (1, 0)])
        mixed = (jnp.where(left, lo, hi) + came.astype(f32)).astype(jnp.bfloat16)
    else:
        mixed = lax.psum_scatter(
            partial.astype(jnp.bfloat16), "head", scatter_dimension=1, tiled=True
        )
    grad_keys, grad_values = (
        jnp.concatenate([pair[i] for pair in gkvs], axis=1) for i in range(2)
    )
    return mixed, jnp.concatenate(gqs, axis=1), grad_keys, grad_values


def solution(mesh):
    both = P("ctx", "head")
    return jax.shard_map(
        per_device,
        mesh=mesh,
        in_specs=(both, both, both, P("head", None), both, P(), P("head")),
        out_specs=(both, both, both, both),
        check_vma=False,
    )
```

```python
import functools
import jax
import jax.numpy as jnp
from jax import lax
from jax.experimental import pallas as pl
from jax.experimental.pallas import tpu as pltpu
from jax.sharding import PartitionSpec as P

HALF = 32
MAXD = 8
FAR = 1e6
NEG = -1e30


def attend_kernel(
    row_count, total, factor, first, index_ref, length_ref, dilation_ref,
    q_ref, go_ref, own_ref, a_ref, b_ref, po_ref, pa_ref,
    att_ref, gq_ref, own_t, a_t, b_t, po_t, pa_t, dist,
):
    slabs = (own_ref, a_ref, b_ref, po_ref, pa_ref)
    outs = (own_t, a_t, b_t, po_t, pa_t)

    @pl.when(pl.program_id(0) == 0)
    def _():
        me = index_ref[0]
        sign = 1 - 2 * lax.rem(me, 2)
        ends = [length_ref[0]]
        for n in range(1, length_ref.shape[0]):
            ends.append(ends[-1] + length_ref[n])

        def segment(pos):
            seg = jnp.zeros(pos.shape, jnp.int32)
            for end in ends:
                seg = seg + (pos >= end).astype(jnp.int32)
            return seg

        qpos = me * row_count + lax.broadcasted_iota(jnp.int32, (1, row_count), 1)
        qseg = segment(qpos)
        for i, off in enumerate((0, 2, -2, 1, -1)):
            kpos = (me + sign * off) * row_count + lax.broadcasted_iota(
                jnp.int32, (row_count, row_count), 0
            )
            same = (segment(kpos) == qseg) & (kpos >= 0) & (kpos < total)
            gap = jnp.abs(kpos - qpos).astype(jnp.float32)
            dist[pl.ds(i * row_count, row_count), :] = jnp.where(same, gap, FAR)

    spacing = jnp.full((1, row_count), dilation_ref[first + pl.program_id(0)], jnp.int32)
    inv = 1.0 / spacing.astype(jnp.float32)
    steps = dist[...] * inv
    whole = jnp.floor(steps + 0.5)
    mask = (whole <= HALF) & (jnp.abs(steps - whole) < 0.01)
    q = q_ref[...]
    go = go_ref[...]
    k = jnp.concatenate([r[0] for r in slabs], axis=0)
    v = jnp.concatenate([r[1] for r in slabs], axis=0)
    nt = (((1,), (1,)), ((), ()))
    tn = (((0,), (0,)), ((), ()))
    f32 = jnp.float32
    scores = lax.dot_general(k, q, nt, preferred_element_type=f32) * factor
    scores = jnp.where(mask, scores, NEG)
    top = jnp.max(scores, axis=0, keepdims=True)
    e = jnp.exp(scores - top)
    w = e * (1.0 / jnp.sum(e, axis=0, keepdims=True))
    p = w.astype(jnp.bfloat16)
    gp = lax.dot_general(v, go, nt, preferred_element_type=f32)
    delta = jnp.sum(w * gp, axis=0, keepdims=True)
    s = (w * (gp - delta)).astype(jnp.bfloat16)
    att_ref[...] = lax.dot_general(p, v, tn, preferred_element_type=f32).astype(jnp.bfloat16)
    gq_ref[...] = (
        lax.dot_general(s, k, tn, preferred_element_type=f32) * factor
    ).astype(jnp.bfloat16)
    kt = (jnp.dot(s, q, preferred_element_type=f32) * factor).astype(jnp.bfloat16)
    vt = jnp.dot(p, go, preferred_element_type=f32).astype(jnp.bfloat16)
    for i, out in enumerate(outs):
        out[0] = kt[i * row_count : (i + 1) * row_count]
        out[1] = vt[i * row_count : (i + 1) * row_count]


def attend(index, lengths, dilation, q, go, slabs, first, total, factor, width):
    rows, cols = q.shape[0], slabs[0].shape[2]
    heads = cols // width
    smem = pl.BlockSpec(memory_space=pltpu.SMEM)
    shared = pl.BlockSpec((rows, width), lambda h: (0, first + h))
    flat = pl.BlockSpec((rows, width), lambda h: (0, h))
    pair = pl.BlockSpec((2, rows, width), lambda h: (0, 0, h))
    one = jax.ShapeDtypeStruct((rows, cols), jnp.bfloat16)
    two = jax.ShapeDtypeStruct((2, rows, cols), jnp.bfloat16)
    return pl.pallas_call(
        functools.partial(attend_kernel, rows, total, factor, first),
        grid=(heads,),
        in_specs=[smem, smem, smem, shared, shared] + [pair] * 5,
        out_specs=[flat, flat] + [pair] * 5,
        out_shape=[one, one] + [two] * 5,
        scratch_shapes=[pltpu.VMEM((5 * rows, rows), jnp.float32)],
        compiler_params=pltpu.CompilerParams(dimension_semantics=("arbitrary",)),
        cost_estimate=pl.CostEstimate(
            flops=heads * 6 * 2 * 5 * rows * rows * width * 8,
            bytes_accessed=24 * 2 * rows * cols,
            transcendentals=heads * 5 * rows * rows,
        ),
    )(index, lengths, dilation, q, go, *slabs)


def per_device(queries, keys, values, out_weight, mixed_grad, lengths, dilation):
    rows = queries.shape[0]
    local_heads = dilation.shape[0]
    width = queries.shape[1] // local_heads
    factor = width ** (-0.5)
    count = lax.axis_size("ctx")
    sides = lax.axis_size("head")
    total = rows * count
    assert 2 * rows >= HALF * MAXD and count % 2 == 0
    index = lax.axis_index("ctx").astype(jnp.int32).reshape(1)

    inward = [
        (j, t) for j in range(count) for t in [j - 2 if j % 2 == 0 else j + 2] if 0 <= t < count
    ]
    outward = [(t, j) for j, t in inward]
    swapped = [(j, j ^ 1) for j in range(count)]

    def move(x, pairs):
        return lax.ppermute(x, "ctx", pairs)

    groups = 1
    gh = local_heads // groups
    cut = [slice(g * gh * width, (g + 1) * gh * width) for g in range(groups)]
    half = mixed_grad.shape[1]
    if sides == 2:
        other = lax.ppermute(mixed_grad, "head", [(0, 1), (1, 0)])
        left = lax.axis_index("head") == 0
        grad_full = jnp.concatenate(
            [jnp.where(left, mixed_grad, other), jnp.where(left, other, mixed_grad)], axis=1
        )
    else:
        grad_full = lax.all_gather(mixed_grad, "head", axis=1, tiled=True)
    stacks = []
    for g in range(groups):
        own = jnp.stack([keys[:, cut[g]], values[:, cut[g]]])
        stacks.append([own, move(own, inward), move(own, outward), move(own, swapped)])
    grad_attention = lax.dot_general(
        grad_full, out_weight, (((1,), (1,)), ((), ())), preferred_element_type=jnp.float32
    ).astype(jnp.bfloat16)

    atts, gqs, gkvs = [], [], []
    f32 = jnp.float32
    for slabs in stacks:
        slabs[1], grad_attention = lax.optimization_barrier((slabs[1], grad_attention))
        slabs.append(move(slabs[1], swapped))
    for g in range(groups):
        att, gq, own_t, a_t, b_t, po_t, pa_t = attend(
            index, lengths, dilation, queries, grad_attention, stacks[g], g * gh, total, factor, width
        )
        pa_back = move(pa_t, swapped)
        b_back = move(b_t, inward)
        po_back = move(po_t, swapped)
        a_sum = (a_t.astype(f32) + pa_back.astype(f32)).astype(jnp.bfloat16)
        a_sum, att = lax.optimization_barrier((a_sum, att))
        a_back = move(a_sum, outward)
        terms = (own_t, po_back, b_back, a_back)
        gkvs.append(
            [sum(term[i].astype(f32) for term in terms).astype(jnp.bfloat16) for i in range(2)]
        )
        atts.append(att)
        gqs.append(gq)
    attention = jnp.concatenate(atts, axis=1)
    partial = jnp.dot(attention, out_weight, preferred_element_type=f32)
    if sides == 2:
        lo, hi = partial[:, :half], partial[:, half:]
        away = jnp.where(left, hi, lo).astype(jnp.bfloat16)
        came = lax.ppermute(away, "head", [(0, 1), (1, 0)])
        mixed = (jnp.where(left, lo, hi) + came.astype(f32)).astype(jnp.bfloat16)
    else:
        mixed = lax.psum_scatter(
            partial.astype(jnp.bfloat16), "head", scatter_dimension=1, tiled=True
        )
    grad_keys, grad_values = (
        jnp.concatenate([pair[i] for pair in gkvs], axis=1) for i in range(2)
    )
    return mixed, jnp.concatenate(gqs, axis=1), grad_keys, grad_values


def solution(mesh):
    both = P("ctx", "head")
    return jax.shard_map(
        per_device,
        mesh=mesh,
        in_specs=(both, both, both, P("head", None), both, P(), P("head")),
        out_specs=(both, both, both, both),
        check_vma=False,
    )
```
